128 devices in a mesh: dp: 16 (over y, z), tp: 8 (over x, core).
Axes of the slice: x: 4, y: 4, z: 4, core: 2. Of those that a mesh axis runs over, the one named last changes fastest.
Arguments:
- x: bfloat16 [16, 1024, 3072], P('dp', 'tp')
- dy: bfloat16 [16, 1024, 3072], P('dp', 'tp')
- wq: bfloat16 [3072, 4096], P('dp', 'tp')
- wk: bfloat16 [3072, 4096], P('dp', 'tp')
- wv: bfloat16 [3072, 4096], P('dp', 'tp')
- wo: bfloat16 [4096, 3072], P(('tp', 'dp'))
- w_gate: bfloat16 [3072, 24576], P('dp', 'tp')
- w_up: bfloat16 [3072, 24576], P('dp', 'tp')
- w_down: bfloat16 [24576, 3072], P(('tp', 'dp'))
Outputs:
- output 1: bfloat16 [16, 1024, 3072], P('dp', 'tp')
- output 2: bfloat16 [3072, 4096], P('dp', 'tp')
- output 3: bfloat16 [3072, 4096], P('dp', 'tp')
- output 4: bfloat16 [3072, 4096], P('dp', 'tp')
- output 5: bfloat16 [4096, 3072], P(('tp', 'dp'))
- output 6: bfloat16 [3072, 24576], P('dp', 'tp')
- output 7: bfloat16 [3072, 24576], P('dp', 'tp')
- output 8: bfloat16 [24576, 3072], P(('tp', 'dp'))
All inputs are finite; a program needn't handle non-finite values.
Results may differ from the reference program's by a relative error of at most 0.024.
Values are sent between devices in bfloat16 or wider.
A program may use at most 1.5 GiB of HBM per device.

```python
import jax
import jax.numpy as jnp
from jax import lax

SEQUENCES = 16
TOKENS = 1024
D = 3072
HEADS = 16
KV_HEADS = 16
HEAD = 256
FF = 24576
THETA = 10000
NAMES = ("wq", "wk", "wv", "wo", "w_gate", "w_up", "w_down")
SHAPES = {
    "wq": (D, HEADS * HEAD),
    "wk": (D, KV_HEADS * HEAD),
    "wv": (D, KV_HEADS * HEAD),
    "wo": (HEADS * HEAD, D),
    "w_gate": (D, FF),
    "w_up": (D, FF),
    "w_down": (FF, D),
}


def bump(key, n, height):
    away = (jnp.arange(n, dtype=jnp.int32) - jax.random.randint(key, (), 0, n, jnp.int32)) % n
    return jnp.where(away < n // 8, height, 1.0)


def together(key, own, strength):
    shared = jax.random.normal(key, own.shape[1:], jnp.float32)
    return (own + strength * shared) * lax.rsqrt(1 + strength * strength)


def setup_inputs(seed: int = 0, part: int = 0) -> dict:
    kx, kdy, ka, kb, kz, kf, kh, kl, *kw = jax.random.split(jax.random.key(seed), 8 + len(NAMES))
    shape = (SEQUENCES, TOKENS, D)
    much_x, much_dy = jax.random.uniform(kz, (2,), jnp.float32, 0.0, 1.0)
    loud = 2.0 ** jax.random.uniform(jax.random.fold_in(kz, 1), (), jnp.float32, -1.0, 2.0)
    halves = 2.0 ** jax.random.uniform(kl, (2,), jnp.float32, -1.0, 1.0)
    times = {"wq": 1.0, "wk": 1.0, "wv": 2.0, "wo": halves[0], "w_gate": 1.0, "w_up": bump(kh, FF, 4.0), "w_down": halves[1]}
    x = together(ka, jax.random.normal(kx, shape, jnp.float32), much_x) * bump(kf, D, 4.0)
    dy = together(kb, jax.random.normal(kdy, shape, jnp.float32), much_dy)
    drawn = {"x": x.astype(jnp.bfloat16), "dy": (loud * dy * (SEQUENCES * TOKENS) ** -0.5).astype(jnp.bfloat16)}
    for key, name in zip(kw, NAMES, strict=True):
        drawn[name] = (jax.random.normal(key, SHAPES[name], jnp.float32) * SHAPES[name][0] ** -0.5 * times[name]).astype(jnp.bfloat16)
    return drawn


def matmul(a, w):
    return jnp.dot(a, w, preferred_element_type=jnp.float32).astype(jnp.bfloat16)


def normed(h):
    wide = h.astype(jnp.float32)
    scale = lax.rsqrt(jnp.mean(wide**2, -1, keepdims=True) + 1e-6)
    return (wide * scale).astype(jnp.bfloat16)


def turned(t, theta):
    half = t.shape[-1] // 2
    angle = jnp.arange(t.shape[0], dtype=jnp.float32)[:, None] * theta ** (-jnp.arange(half, dtype=jnp.float32) / half)
    cos, sin = jnp.cos(angle)[:, None], jnp.sin(angle)[:, None]
    a, b = t[..., :half].astype(jnp.float32), t[..., half:].astype(jnp.float32)
    return jnp.concatenate([a * cos - b * sin, b * cos + a * sin], -1).astype(jnp.bfloat16)


def seen_by(q, k, v):
    tokens, kv = q.shape[0], k.shape[1]
    q = q.reshape(tokens, kv, -1, q.shape[-1])
    scores = jnp.einsum("tgsd,ugd->gstu", q.astype(jnp.float32), k.astype(jnp.float32)) * q.shape[-1] ** -0.5
    place = jnp.arange(tokens)
    weights = jax.nn.softmax(jnp.where(place[:, None] >= place, scores, -jnp.inf), -1).astype(jnp.bfloat16)
    return jnp.einsum("gstu,ugd->tgsd", weights.astype(jnp.float32), v.astype(jnp.float32)).astype(jnp.bfloat16).reshape(tokens, -1)


def layer(h, w):
    a = normed(h)
    q, k = (turned(matmul(a, w[name]).reshape(h.shape[0], -1, HEAD), THETA) for name in ("wq", "wk"))
    h = h + matmul(seen_by(q, k, matmul(a, w["wv"]).reshape(h.shape[0], -1, HEAD)), w["wo"])
    b = normed(h)
    gate = jnp.dot(b, w["w_gate"], preferred_element_type=jnp.float32)
    up = jnp.dot(b, w["w_up"], preferred_element_type=jnp.float32)
    return h + matmul((jax.nn.silu(gate) * up).astype(jnp.bfloat16), w["w_down"])


def reference(x, dy, wq, wk, wv, wo, w_gate, w_up, w_down):
    weights = dict(zip(NAMES, (wq, wk, wv, wo, w_gate, w_up, w_down), strict=True))

    def take(so_far, sequence):
        h, by_y = sequence
        _, back = jax.vjp(lambda w, h: layer(h, w), weights, h)
        by_weights, by_h = back(by_y)
        return jax.tree.map(lambda total, term: total + term.astype(jnp.float32), so_far, by_weights), by_h

    none_yet = {name: jnp.zeros(w.shape, jnp.float32) for name, w in weights.items()}
    by_weights, by_x = lax.scan(take, none_yet, (x, dy))
    return (by_x, *(by_weights[name].astype(jnp.bfloat16) for name in NAMES))
```

```python
import functools

import jax
import jax.numpy as jnp
from jax import lax
from jax.experimental import pallas as pl
from jax.experimental.layout import Layout, with_layout_constraint
from jax.experimental.pallas import tpu as pltpu
from jax.sharding import PartitionSpec as P

HEAD = 256
HALF = HEAD // 2
THETA = 10000
LOG2E = 1.4426950408889634
HIDDEN = -2e30
VMEM = 56 * 2**20
STRIP = 256
TILE = 256
SIDE = 4
CORES = 2
SHARDS = SIDE * CORES
PLACES = SIDE * SIDE
BF16, F32 = jnp.bfloat16, jnp.float32


def dot(a, b, ca=1, cb=0):
    return lax.dot_general(a, b, (((ca,), (cb,)), ((), ())), preferred_element_type=F32)


def matmul(a, b, ca=1, cb=0):
    return dot(a, b, ca, cb).astype(BF16)


def row_major(t):
    return with_layout_constraint(t, Layout(major_to_minor=tuple(range(t.ndim))))


def normed(h):
    wide = h.astype(F32)
    scale = lax.rsqrt(jnp.mean(wide**2, -1, keepdims=True) + 1e-6)
    return (wide * scale).astype(BF16)


def shaped(*shape):
    return jax.ShapeDtypeStruct(shape, BF16)


def call(body, grid, ins, outs, tables=(), scratch=(), flops=0):
    moved = sum(t.size * t.dtype.itemsize for t, _, _ in [*ins, *outs])
    return pl.pallas_call(
        body,
        grid_spec=pltpu.PrefetchScalarGridSpec(
            num_scalar_prefetch=len(tables), grid=(grid,), in_specs=[pl.BlockSpec(b, m) for _, b, m in ins],
            out_specs=[pl.BlockSpec(b, m) for _, b, m in outs], scratch_shapes=list(scratch)),
        out_shape=[s for s, _, _ in outs],
        compiler_params=pltpu.CompilerParams(dimension_semantics=("arbitrary",), vmem_limit_bytes=VMEM),
        cost_estimate=pl.CostEstimate(flops=flops or 100 * moved, transcendentals=0, bytes_accessed=moved),
    )(*tables, *[t for t, _, _ in ins])


def _scores(q_ref, k_ref, at):
    seen = at + STRIP
    s = dot(k_ref[:seen, :], q_ref[at:seen, :], 1, 1)
    key, query = (lax.broadcasted_iota(jnp.int32, s.shape, n) for n in range(2))
    return jnp.where(key <= query + at, s, HIDDEN)


def _forward(q_ref, k_ref, v_ref, o_ref, lse_ref):
    scale = HEAD**-0.5
    for at in range(0, q_ref.shape[0], STRIP):
        seen = at + STRIP
        s = _scores(q_ref, k_ref, at)
        top = s.max(axis=0, keepdims=True)
        p = jnp.exp2((s - top) * (scale * LOG2E)).astype(BF16)
        values = jnp.concatenate([v_ref[:seen, :].T, jnp.ones((8, seen), BF16)], axis=0)
        mix = dot(values, p)
        total = mix[HEAD : HEAD + 1, :]
        o_ref[at:seen, :] = (mix[:HEAD, :] * (1 / total)).T.astype(BF16)
        lse_ref[0, :, at:seen] = top * scale + jnp.log(total)


def _backward(q_ref, k_ref, v_ref, do_ref, lse_ref, delta_ref, dq_ref, dk_ref, dv_ref, dk_s, dv_s):
    scale = HEAD**-0.5
    dk_s[...] = jnp.zeros_like(dk_s)
    dv_s[...] = jnp.zeros_like(dv_s)
    for at in range(0, q_ref.shape[0], STRIP):
        seen = at + STRIP
        q, do = q_ref[at:seen, :], do_ref[at:seen, :]
        p = jnp.exp2(_scores(q_ref, k_ref, at) * (scale * LOG2E) - lse_ref[0, :, at:seen] * LOG2E)
        ds = (p * (dot(v_ref[:seen, :], do, 1, 1) - delta_ref[0, :, at:seen])).astype(BF16)
        dv_s[:seen, :] += dot(p.astype(BF16), do)
        dk_s[:seen, :] += dot(ds, q)
        dq_ref[at:seen, :] = (dot(k_ref[:seen, :].T, ds) * scale).T.astype(BF16)
    dk_ref[...] = (dk_s[...] * scale).astype(BF16)
    dv_ref[...] = dv_s[...].astype(BF16)


def attend(qkv):
    s, h = qkv.shape[0], qkv.shape[1] // (3 * HEAD)
    cols = lambda n: (qkv, (s, HEAD), lambda i: (0, n * h + i))
    return call(_forward, h, [cols(0), cols(1), cols(2)],
                [(shaped(s, h * HEAD), (s, HEAD), lambda i: (0, i)), (jax.ShapeDtypeStruct((h, 1, s), F32), (1, 1, s), lambda i: (i, 0, 0))],
                flops=4 * s * s * h * HEAD)


def attend_back(qkv, d_out, lse, delta):
    s, h = qkv.shape[0], qkv.shape[1] // (3 * HEAD)
    cols = lambda n: (qkv, (s, HEAD), lambda i: (0, n * h + i))
    one = lambda t: (t, (s, HEAD), lambda i: (0, i))
    stat = lambda t: (t, (1, 1, s), lambda i: (i, 0, 0))
    return call(_backward, h, [cols(0), cols(1), cols(2), one(d_out), stat(lse), stat(delta)], 3 * [one(shaped(s, h * HEAD))],
                scratch=2 * [pltpu.VMEM((s, HEAD), F32)], flops=10 * s * s * h * HEAD)


def _beside(a_ref, b_ref, out_ref):
    out_ref[:, :TILE] = a_ref[...]
    out_ref[:, TILE:] = b_ref[...]


def _apart(t_ref, a_ref, b_ref):
    a_ref[...] = t_ref[:, :TILE]
    b_ref[...] = t_ref[:, TILE:]


def _column(t, wide):
    return t, (t.shape[0], wide), lambda i: (0, i)


def beside(a, b):
    rows, n = a.shape
    return call(_beside, n // TILE, [_column(a, TILE), _column(b, TILE)], [_column(shaped(rows, 2 * n), 2 * TILE)])[0]


def apart(t):
    rows, n = t.shape[0], t.shape[1] // 2
    return call(_apart, n // TILE, [_column(t, 2 * TILE)], 2 * [_column(shaped(rows, n), TILE)])


def _into(b_ref, w_ref, both_ref, hidden_ref):
    both = dot(b_ref[...], w_ref[...])
    both_ref[...] = both
    hidden_ref[...] = (jax.nn.silu(both[:, :TILE]) * both[:, TILE:]).astype(BF16)


def into_hidden(b, w):
    m, k, n = *b.shape, w.shape[1]
    return call(_into, n // (2 * TILE), [(b, b.shape, lambda i: (0, 0)), _column(w, 2 * TILE)],
                [_column(jax.ShapeDtypeStruct((m, n), F32), 2 * TILE), _column(shaped(m, n // 2), TILE)], flops=2 * m * k * n)


def _back_into(d_ref, w_ref, both_ref, out_ref):
    d = matmul(d_ref[...], w_ref[...], 1, 1).astype(F32)
    gate, up = both_ref[:, :TILE], both_ref[:, TILE:]
    s = jax.nn.sigmoid(gate)
    out_ref[:, :TILE] = (d * up * (s * (1 + gate * (1 - s)))).astype(BF16)
    out_ref[:, TILE:] = (d * (gate * s)).astype(BF16)


def hidden_back(d, w, both):
    m, k, n = *d.shape, w.shape[0]
    return call(_back_into, n // TILE, [(d, d.shape, lambda i: (0, 0)), (w, (TILE, k), lambda i: (i, 0)), _column(both, 2 * TILE)],
                [_column(shaped(m, 2 * n), 2 * TILE)], flops=2 * m * k * n)[0]


def along_x(i):
    return "tp", [(t, (t + CORES * i) % SHARDS) for t in range(SHARDS)]


def along_y(i):
    return "dp", [(p, (p + SIDE * i) % PLACES) for p in range(PLACES)]


def along_z(i):
    return "dp", [(p, p // SIDE * SIDE + (p + i) % SIDE) for p in range(PLACES)]


def swap():
    return "tp", [(t, t + 1 - 2 * (t % CORES)) for t in range(SHARDS)]


def send(t, way):
    return lax.ppermute(t, *way)


def gather_tokens(t):
    mine = jnp.concatenate([t] + [send(t, along_x(-i)) for i in range(1, SIDE)])
    return jnp.concatenate([mine, send(mine, swap())])


def scatter_tokens(t, w, cw):
    half = t.shape[0] // CORES
    other = send(matmul(t[half:], w, 1, cw), swap())
    chip = matmul(t[:half], w, 1, cw).astype(F32) + other.astype(F32)
    parts = jnp.split(chip, SIDE)
    total = parts[0]
    for i in range(1, SIDE):
        total += send(parts[i].astype(BF16), along_x(i)).astype(F32)
    return total.astype(BF16)


def orders():
    me = lax.axis_index("tp")
    chip, core = me // CORES, me % CORES
    run = jnp.arange(SHARDS, dtype=jnp.int32)
    lies_at = SIDE * ((run % CORES + core) % CORES) + (run // CORES + SIDE - chip) % SIDE
    holds = CORES * ((run % SIDE + chip) % SIDE) + (run // SIDE + core) % CORES
    return lies_at, holds


def _turn(t, cos, sin):
    done = []
    for at in range(0, t.shape[1], HEAD):
        a, b = t[:, at : at + HALF].astype(F32), t[:, at + HALF : at + HEAD].astype(F32)
        done += [a * cos - b * sin, b * cos + a * sin]
    return jnp.concatenate(done, 1).astype(BF16)


def _ordered(_, t_ref, cos_ref, sin_ref, out_ref):
    turned = 2 * t_ref.shape[1] // 3
    out_ref[:, :turned] = _turn(t_ref[:, :turned], cos_ref[...], sin_ref[...])
    out_ref[:, turned:] = t_ref[:, turned:]


def _given_back(_, q_ref, k_ref, v_ref, cos_ref, sin_ref, out_ref):
    n = q_ref.shape[1]
    out_ref[:, :n] = _turn(q_ref[...], cos_ref[...], -sin_ref[...])
    out_ref[:, n : 2 * n] = _turn(k_ref[...], cos_ref[...], -sin_ref[...])
    out_ref[:, 2 * n :] = v_ref[...]


def _copied(_, t_ref, out_ref):
    out_ref[...] = t_ref[...]


def _with_delta(_, do_ref, o_ref, out_ref, delta_ref):
    out_ref[...] = do_ref[...]
    both = do_ref[...].astype(F32) * o_ref[...].astype(F32)
    for n in range(delta_ref.shape[0]):
        delta_ref[n] = both[:, n * HEAD : (n + 1) * HEAD].T.sum(axis=0, keepdims=True)


def run_at(t, by_table):
    return t, (t.shape[0] // SHARDS, t.shape[1]), (lambda i, at: (at[i], 0)) if by_table else (lambda i, at: (i, 0))


def ring_gather(t, way):
    half = t.shape[0] // 2
    before, after = send(t, way(1)), send(t, way(-1))
    return jnp.concatenate([t, after, send(before[:half], way(1)), send(after[half:], way(-1)), before])


def ring_scatter(t, way):
    rows = t.shape[0] // SIDE
    half = rows // 2
    own, right, far, left = (t[n * rows : (n + 1) * rows] for n in range(SIDE))
    add = lambda a, b: (a.astype(F32) + b.astype(F32)).astype(BF16)
    right_more, left_more = send(far[:half].astype(BF16), way(1)), send(far[half:].astype(BF16), way(-1))
    right = jnp.concatenate([add(right[:half], right_more), right[half:].astype(BF16)])
    left = jnp.concatenate([left[:half].astype(BF16), add(left[half:], left_more)])
    return own.astype(F32) + send(right, way(1)).astype(F32) + send(left, way(-1)).astype(F32)


def places():
    me = lax.axis_index("dp")
    y, z = me // SIDE, me % SIDE
    n = jnp.arange(PLACES, dtype=jnp.int32)
    high, low = n // SIDE, n % SIDE
    dy, dz = (high + SIDE - y) % SIDE, (low + SIDE - z) % SIDE
    return (SIDE * dz + dy, SIDE * dy + dz), (SIDE * ((low + y) % SIDE) + (high + z) % SIDE, SIDE * ((high + y) % SIDE) + (low + z) % SIDE)


def _placed(*refs):
    halves, (qkv_ref, o_ref) = refs[2:4], refs[4:]
    tall, low = qkv_ref.shape[0], o_ref.shape[0]
    wide = halves[0].shape[1]
    for n, ref in enumerate(halves):
        qkv_ref[:, n * wide : (n + 1) * wide] = ref[:tall, :]
        for i in range(o_ref.shape[1] // (2 * wide)):
            o_ref[:, (2 * i + n) * wide : (2 * i + n + 1) * wide] = ref[tall + i * low : tall + (i + 1) * low, :]


def attn_shard(halves, tall, low, many):
    cols = 2 * halves[0].shape[1]
    block = (tall + low * many, cols // 2)
    return call(_placed, PLACES, [(halves[0], block, lambda i, a, b: (a[i], 0)), (halves[1], block, lambda i, a, b: (b[i], 0))],
                [(shaped(PLACES * tall, cols), (tall, cols), lambda i, a, b: (i, 0)), (shaped(PLACES * low, cols * many), (low, cols * many), lambda i, a, b: (i, 0))],
                places()[0])


def _packed(*refs):
    ins, outs = refs[2:-2], refs[-2:]
    many = len(ins) // 2 - 1
    for n, ref in enumerate(outs):
        tall = ins[0].shape[0]
        ref[:tall, :] = ins[n][...]
        for i in range(many):
            low = ins[2].shape[0]
            ref[tall + i * low : tall + (i + 1) * low, :] = ins[2 + 2 * i + n][...]


def attn_pack(by_qkv, by_o):
    tall, low = by_qkv.shape[0] // PLACES, by_o.shape[0] // PLACES
    wide = by_qkv.shape[1] // 2
    many = by_o.shape[1] // (2 * wide)
    spot = lambda n, column: (lambda i, a, b: ((a, b)[n][i], column))
    ins = [(by_qkv, (tall, wide), spot(n, n)) for n in range(2)]
    ins += [(by_o, (low, wide), spot(n, 2 * m + n)) for m in range(many) for n in range(2)]
    rows = tall + many * low
    return call(_packed, PLACES, ins, 2 * [(shaped(PLACES * rows, wide), (rows, wide), lambda i, a, b: (i, 0))], places()[1])


def solution(mesh):
    def whole(t):
        return lax.all_gather(t, "dp", axis=0, tiled=True)

    def summed(t):
        return lax.psum_scatter(t, "dp", scatter_dimension=0, tiled=True)

    def step(x, dy, wq, wk, wv, wo, w_gate, w_up, w_down):
        h, dy = x[0], dy[0]
        tall, low, cols = wq.shape[0], wo.shape[0], 3 * wq.shape[1]
        many = wo.shape[1] // cols
        attn = jnp.concatenate([jnp.concatenate([wq, wk, wv], 1)] + [wo[:, i * cols : (i + 1) * cols] for i in range(many)])
        halves = ring_gather(ring_gather(attn[:, : cols // 2], along_y), along_z), ring_gather(ring_gather(attn[:, cols // 2 :], along_z), along_y)
        w_qkv, w_o = attn_shard(halves, tall, low, many)
        w_in = whole(beside(w_gate, w_up))
        w_out = whole(w_down)

        tokens = SHARDS * h.shape[0]
        lies_at, holds = orders()
        angle = jnp.arange(tokens, dtype=F32)[:, None] * THETA ** (-jnp.arange(HALF, dtype=F32) / HALF)
        cos, sin = jnp.cos(angle), jnp.sin(angle)

        a_own, norm_a = jax.vjp(normed, h)
        a = gather_tokens(a_own)
        d_y = gather_tokens(dy)
        qkv = call(_ordered, SHARDS, [run_at(matmul(a, w_qkv), True), run_at(cos, False), run_at(sin, False)], [run_at(shaped(tokens, cols), False)], (lies_at,))[0]
        out, lse = attend(qkv)
        heads = call(_copied, SHARDS, [run_at(out, True)], [run_at(shaped(*out.shape), False)], (holds,))[0]
        h = h + scatter_tokens(heads, w_o, 0)
        b_own, norm_b = jax.vjp(normed, h)
        b = gather_tokens(b_own)
        both, hidden = into_hidden(b, w_in)

        d_out_w, w_out = lax.optimization_barrier((row_major(matmul(hidden, d_y, 0, 0)), w_out))
        by_out = summed(d_out_w)
        d_both = hidden_back(d_y, w_out, both)
        d_in_w, d_both = lax.optimization_barrier((row_major(matmul(b, d_both, 0, 0)), d_both))
        by_in = summed(d_in_w)
        d_b, by_out = lax.optimization_barrier((scatter_tokens(d_both, w_in, 1), by_out))
        d_h = dy + norm_b(d_b)[0]
        d_attn = gather_tokens(d_h)
        d_out, delta = call(_with_delta, SHARDS, [run_at(matmul(d_attn, w_o, 1, 1), True), run_at(out, False)],
                            [run_at(shaped(*out.shape), False), (jax.ShapeDtypeStruct(lse.shape, F32), (*lse.shape[:2], h.shape[0]), lambda i, at: (0, 0, i))],
                            (lies_at,))
        by_o = row_major(matmul(heads, d_attn, 0, 0))
        d_qkv = call(_given_back, SHARDS, [run_at(t, True) for t in (*attend_back(qkv, d_out, lse, delta), cos, sin)], [run_at(shaped(*qkv.shape), False)], (holds,))[0]
        first, second = attn_pack(row_major(matmul(a, d_qkv, 0, 0)), by_o)
        first, second, d_qkv = lax.optimization_barrier((first, second, d_qkv))
        first, second = ring_scatter(ring_scatter(first, along_z), along_y), ring_scatter(ring_scatter(second, along_y), along_z)
        d_x = d_h + norm_a(scatter_tokens(d_qkv, w_qkv, 1))[0]
        by_attn = jnp.concatenate([first, second], 1).astype(BF16)
        by_o = jnp.concatenate([by_attn[tall + i * low : tall + (i + 1) * low] for i in range(many)], 1)
        return (d_x[None], *jnp.split(by_attn[:tall], 3, 1), by_o, *apart(by_in), by_out)

    states, by_columns, by_rows = P("dp", "tp", None), P("dp", "tp"), P(("tp", "dp"), None)
    weights = (by_columns, by_columns, by_columns, by_rows, by_columns, by_columns, by_rows)
    return jax.shard_map(step, mesh=mesh, in_specs=(states, states, *weights), out_specs=(states, *weights), check_vma=False)
```

```python
import functools

import jax
import jax.numpy as jnp
from jax import lax
from jax.experimental import pallas as pl
from jax.experimental.layout import Layout, with_layout_constraint
from jax.experimental.pallas import tpu as pltpu
from jax.sharding import PartitionSpec as P

HEAD = 256
HALF = HEAD // 2
THETA = 10000
LOG2E = 1.4426950408889634
HIDDEN = -2e30
VMEM = 56 * 2**20
STRIP = 256
TILE = 256
SIDE = 4
CORES = 2
SHARDS = SIDE * CORES
PLACES = SIDE * SIDE
BF16, F32 = jnp.bfloat16, jnp.float32


def dot(a, b, ca=1, cb=0):
    return lax.dot_general(a, b, (((ca,), (cb,)), ((), ())), preferred_element_type=F32)


def matmul(a, b, ca=1, cb=0):
    return dot(a, b, ca, cb).astype(BF16)


def row_major(t):
    return with_layout_constraint(t, Layout(major_to_minor=tuple(range(t.ndim))))


def normed(h):
    wide = h.astype(F32)
    scale = lax.rsqrt(jnp.mean(wide**2, -1, keepdims=True) + 1e-6)
    return (wide * scale).astype(BF16)


def shaped(*shape):
    return jax.ShapeDtypeStruct(shape, BF16)


def call(body, grid, ins, outs, tables=(), scratch=(), flops=0):
    moved = sum(t.size * t.dtype.itemsize for t, _, _ in [*ins, *outs])
    return pl.pallas_call(
        body,
        grid_spec=pltpu.PrefetchScalarGridSpec(
            num_scalar_prefetch=len(tables), grid=(grid,), in_specs=[pl.BlockSpec(b, m) for _, b, m in ins],
            out_specs=[pl.BlockSpec(b, m) for _, b, m in outs], scratch_shapes=list(scratch)),
        out_shape=[s for s, _, _ in outs],
        compiler_params=pltpu.CompilerParams(dimension_semantics=("arbitrary",), vmem_limit_bytes=VMEM),
        cost_estimate=pl.CostEstimate(flops=flops or 100 * moved, transcendentals=0, bytes_accessed=moved),
    )(*tables, *[t for t, _, _ in ins])


def all_of(t):
    return t, t.shape, lambda *_: (0,) * len(t.shape)


def _scores(q_ref, k_ref, at):
    seen = at + STRIP
    s = dot(k_ref[:seen, :], q_ref[at:seen, :], 1, 1)
    key, query = (lax.broadcasted_iota(jnp.int32, s.shape, n) for n in range(2))
    return jnp.where(key <= query + at, s, HIDDEN)


def _forward(q_ref, k_ref, v_ref, o_ref, lse_ref):
    scale = HEAD**-0.5
    for at in range(0, q_ref.shape[0], STRIP):
        seen = at + STRIP
        s = _scores(q_ref, k_ref, at)
        top = s.max(axis=0, keepdims=True)
        p = jnp.exp2((s - top) * (scale * LOG2E)).astype(BF16)
        values = jnp.concatenate([v_ref[:seen, :].T, jnp.ones((8, seen), BF16)], axis=0)
        mix = dot(values, p)
        total = mix[HEAD : HEAD + 1, :]
        o_ref[at:seen, :] = (mix[:HEAD, :] * (1 / total)).T.astype(BF16)
        lse_ref[0, :, at:seen] = top * scale + jnp.log(total)


def _backward(q_ref, k_ref, v_ref, do_ref, lse_ref, delta_ref, dq_ref, dk_ref, dv_ref, dk_s, dv_s):
    scale = HEAD**-0.5
    dk_s[...] = jnp.zeros_like(dk_s)
    dv_s[...] = jnp.zeros_like(dv_s)
    for at in range(0, q_ref.shape[0], STRIP):
        seen = at + STRIP
        q, do = q_ref[at:seen, :], do_ref[at:seen, :]
        p = jnp.exp2(_scores(q_ref, k_ref, at) * (scale * LOG2E) - lse_ref[0, :, at:seen] * LOG2E)
        ds = (p * (dot(v_ref[:seen, :], do, 1, 1) - delta_ref[0, :, at:seen])).astype(BF16)
        dv_s[:seen, :] += dot(p.astype(BF16), do)
        dk_s[:seen, :] += dot(ds, q)
        dq_ref[at:seen, :] = (dot(k_ref[:seen, :].T, ds) * scale).T.astype(BF16)
    dk_ref[...] = (dk_s[...] * scale).astype(BF16)
    dv_ref[...] = dv_s[...].astype(BF16)


def attend(qkv):
    s, h = qkv.shape[0], qkv.shape[1] // (3 * HEAD)
    cols = lambda n: (qkv, (s, HEAD), lambda i: (0, n * h + i))
    return call(_forward, h, [cols(0), cols(1), cols(2)],
                [(shaped(s, h * HEAD), (s, HEAD), lambda i: (0, i)), (jax.ShapeDtypeStruct((h, 1, s), F32), (1, 1, s), lambda i: (i, 0, 0))],
                flops=4 * s * s * h * HEAD)


def attend_back(qkv, d_out, lse, delta):
    s, h = qkv.shape[0], qkv.shape[1] // (3 * HEAD)
    cols = lambda n: (qkv, (s, HEAD), lambda i: (0, n * h + i))
    one = lambda t: (t, (s, HEAD), lambda i: (0, i))
    stat = lambda t: (t, (1, 1, s), lambda i: (i, 0, 0))
    return call(_backward, h, [cols(0), cols(1), cols(2), one(d_out), stat(lse), stat(delta)], 3 * [one(shaped(s, h * HEAD))],
                scratch=2 * [pltpu.VMEM((s, HEAD), F32)], flops=10 * s * s * h * HEAD)


def _beside(a_ref, b_ref, out_ref):
    for at in range(0, a_ref.shape[1], TILE):
        out_ref[:, 2 * at : 2 * at + TILE] = a_ref[:, at : at + TILE]
        out_ref[:, 2 * at + TILE : 2 * (at + TILE)] = b_ref[:, at : at + TILE]


def _apart(t_ref, a_ref, b_ref):
    for at in range(0, a_ref.shape[1], TILE):
        a_ref[:, at : at + TILE] = t_ref[:, 2 * at : 2 * at + TILE]
        b_ref[:, at : at + TILE] = t_ref[:, 2 * at + TILE : 2 * (at + TILE)]


def _column(t, wide):
    return t, (t.shape[0], wide), lambda i: (0, i)


def beside(a, b):
    rows, n = a.shape
    return call(_beside, 1, [all_of(a), all_of(b)], [all_of(shaped(rows, 2 * n))])[0]


def apart(t):
    rows, n = t.shape[0], t.shape[1] // 2
    return call(_apart, 1, [all_of(t)], 2 * [all_of(shaped(rows, n))])


def _into(b_ref, w_ref, both_ref, hidden_ref):
    both = dot(b_ref[...], w_ref[...])
    both_ref[...] = both
    hidden_ref[...] = (jax.nn.silu(both[:, :TILE]) * both[:, TILE:]).astype(BF16)


def into_hidden(b, w):
    m, k, n = *b.shape, w.shape[1]
    return call(_into, n // (2 * TILE), [all_of(b), _column(w, 2 * TILE)],
                [_column(jax.ShapeDtypeStruct((m, n), F32), 2 * TILE), _column(shaped(m, n // 2), TILE)], flops=2 * m * k * n)


def _back_into(d_ref, w_ref, both_ref, out_ref):
    d = matmul(d_ref[...], w_ref[...], 1, 1).astype(F32)
    gate, up = both_ref[:, :TILE], both_ref[:, TILE:]
    s = jax.nn.sigmoid(gate)
    out_ref[:, :TILE] = (d * up * (s * (1 + gate * (1 - s)))).astype(BF16)
    out_ref[:, TILE:] = (d * (gate * s)).astype(BF16)


def hidden_back(d, w, both):
    m, k, n = *d.shape, w.shape[0]
    return call(_back_into, n // TILE, [all_of(d), (w, (TILE, k), lambda i: (i, 0)), _column(both, 2 * TILE)],
                [_column(shaped(m, 2 * n), 2 * TILE)], flops=2 * m * k * n)[0]


def along_x(i):
    return "tp", [(t, (t + CORES * i) % SHARDS) for t in range(SHARDS)]


def along_y(i):
    return "dp", [(p, (p + SIDE * i) % PLACES) for p in range(PLACES)]


def along_z(i):
    return "dp", [(p, p // SIDE * SIDE + (p + i) % SIDE) for p in range(PLACES)]


def swap():
    return "tp", [(t, t + 1 - 2 * (t % CORES)) for t in range(SHARDS)]


def send(t, way):
    return lax.ppermute(t, *way)


def gather_tokens(t):
    mine = [t] + [send(t, along_x(-i)) for i in range(1, SIDE)]
    return jnp.concatenate(mine + [send(block, swap()) for block in mine])


def chip_sum(t, w, cw):
    half = t.shape[0] // CORES
    other = send(matmul(t[half:], w, 1, cw), swap())
    own, *others = jnp.split(matmul(t[:half], w, 1, cw).astype(F32) + other.astype(F32), SIDE)
    return own, [t.astype(BF16) for t in others]


def place_sum(own, others):
    for i, t in enumerate(others):
        own += send(t, along_x(i + 1)).astype(F32)
    return own.astype(BF16)


def scatter_tokens(t, w, cw):
    return place_sum(*chip_sum(t, w, cw))


def orders():
    me = lax.axis_index("tp")
    chip, core = me // CORES, me % CORES
    run = jnp.arange(SHARDS, dtype=jnp.int32)
    lies_at = SIDE * ((run % CORES + core) % CORES) + (run // CORES + SIDE - chip) % SIDE
    holds = CORES * ((run % SIDE + chip) % SIDE) + (run // SIDE + core) % CORES
    return lies_at, holds


def _turn(t, cos, sin):
    done = []
    for at in range(0, t.shape[1], HEAD):
        a, b = t[:, at : at + HALF].astype(F32), t[:, at + HALF : at + HEAD].astype(F32)
        done += [a * cos - b * sin, b * cos + a * sin]
    return jnp.concatenate(done, 1).astype(BF16)


def _runs(at, n):
    return [(pl.ds(pl.multiple_of(at[i] * n, n), n), slice(i * n, (i + 1) * n)) for i in range(SHARDS)]


def _ordered(at, t_ref, cos_ref, sin_ref, out_ref):
    turned = 2 * t_ref.shape[1] // 3
    for there, here in _runs(at, t_ref.shape[0] // SHARDS):
        out_ref[here, :turned] = _turn(t_ref[there, :turned], cos_ref[here, :], sin_ref[here, :])
        out_ref[here, turned:] = t_ref[there, turned:]


def _given_back(at, q_ref, k_ref, v_ref, cos_ref, sin_ref, out_ref):
    n = q_ref.shape[1]
    for there, here in _runs(at, q_ref.shape[0] // SHARDS):
        cos, sin = cos_ref[there, :], -sin_ref[there, :]
        out_ref[here, :n] = _turn(q_ref[there, :], cos, sin)
        out_ref[here, n : 2 * n] = _turn(k_ref[there, :], cos, sin)
        out_ref[here, 2 * n :] = v_ref[there, :]


def _copied(at, t_ref, out_ref):
    for there, here in _runs(at, t_ref.shape[0] // SHARDS):
        out_ref[here, :] = t_ref[there, :]


def _with_delta(at, do_ref, o_ref, out_ref, delta_ref):
    for there, here in _runs(at, do_ref.shape[0] // SHARDS):
        do = do_ref[there, :]
        out_ref[here, :] = do
        both = do.astype(F32) * o_ref[here, :].astype(F32)
        for n in range(delta_ref.shape[0]):
            delta_ref[n, :, here] = both[:, n * HEAD : (n + 1) * HEAD].T.sum(axis=0, keepdims=True)


def moved(body, table, ins, outs):
    return call(body, 1, [all_of(t) for t in ins], [all_of(t) for t in outs], (table,))


def ring_gather(t, way):
    half = t.shape[0] // 2
    before, after = send(t, way(1)), send(t, way(-1))
    return jnp.concatenate([t, after, send(before[:half], way(1)), send(after[half:], way(-1)), before])


def ring_far(t, way):
    half = t.shape[0] // (2 * SIDE)
    far = t[2 * 2 * half : 3 * 2 * half].astype(BF16)
    return t, send(far[:half], way(1)), send(far[half:], way(-1))


def ring_near(t, before, after, way):
    rows = t.shape[0] // SIDE
    half = rows // 2
    own, right, _, left = (t[n * rows : (n + 1) * rows] for n in range(SIDE))
    add = lambda a, b: (a.astype(F32) + b.astype(F32)).astype(BF16)
    right = jnp.concatenate([add(right[:half], before), right[half:].astype(BF16)])
    left = jnp.concatenate([left[:half].astype(BF16), add(left[half:], after)])
    return own.astype(F32) + send(right, way(1)).astype(F32) + send(left, way(-1)).astype(F32)


def ring_scatter(t, way):
    return ring_near(*ring_far(t, way), way)


def places():
    me = lax.axis_index("dp")
    y, z = me // SIDE, me % SIDE
    n = jnp.arange(PLACES, dtype=jnp.int32)
    high, low = n // SIDE, n % SIDE
    dy, dz = (high + SIDE - y) % SIDE, (low + SIDE - z) % SIDE
    return (SIDE * dz + dy, SIDE * dy + dz), (SIDE * ((low + y) % SIDE) + (high + z) % SIDE, SIDE * ((high + y) % SIDE) + (low + z) % SIDE)


def _placed(*refs):
    halves, (qkv_ref, o_ref) = refs[2:4], refs[4:]
    tall, low = qkv_ref.shape[0], o_ref.shape[0]
    wide = halves[0].shape[1]
    for n, ref in enumerate(halves):
        qkv_ref[:, n * wide : (n + 1) * wide] = ref[:tall, :]
        for i in range(o_ref.shape[1] // (2 * wide)):
            o_ref[:, (2 * i + n) * wide : (2 * i + n + 1) * wide] = ref[tall + i * low : tall + (i + 1) * low, :]


def attn_shard(halves, tall, low, many):
    cols = 2 * halves[0].shape[1]
    block = (tall + low * many, cols // 2)
    return call(_placed, PLACES, [(halves[0], block, lambda i, a, b: (a[i], 0)), (halves[1], block, lambda i, a, b: (b[i], 0))],
                [(shaped(PLACES * tall, cols), (tall, cols), lambda i, a, b: (i, 0)), (shaped(PLACES * low, cols * many), (low, cols * many), lambda i, a, b: (i, 0))],
                places()[0])


def _packed(first, second, qkv_ref, o_ref, *outs):
    tall, low = qkv_ref.shape[0] // PLACES, o_ref.shape[0] // PLACES
    spots = PLACES // pl.num_programs(0)
    for n, (at, ref) in enumerate(zip((first, second), outs)):
        wide = ref.shape[1]
        for spot in range(PLACES // SIDE):
            place = at[pl.program_id(0) * spots + spot]
            row = spot * (ref.shape[0] // SIDE)
            ref[row : row + tall, :] = qkv_ref[pl.ds(pl.multiple_of(place * tall, tall), tall), n * wide : (n + 1) * wide]
            row += tall
            for i in range(o_ref.shape[1] // (2 * wide)):
                ref[row : row + low, :] = o_ref[pl.ds(pl.multiple_of(place * low, low), low), (2 * i + n) * wide : (2 * i + n + 1) * wide]
                row += low


def attn_pack(by_qkv, by_o):
    wide = by_qkv.shape[1] // 2
    rows = (by_qkv.size + by_o.size) // (2 * wide)
    return call(_packed, SIDE, [all_of(by_qkv), all_of(by_o)], 2 * [(shaped(rows, wide), (rows // SIDE, wide), lambda i, *_: (i, 0))], places()[1])


def solution(mesh):
    def whole(t):
        return lax.all_gather(t, "dp", axis=0, tiled=True)

    def summed(t):
        return lax.psum_scatter(t, "dp", scatter_dimension=0, tiled=True)

    def step(x, dy, wq, wk, wv, wo, w_gate, w_up, w_down):
        h, dy = x[0], dy[0]
        tall, low, cols = wq.shape[0], wo.shape[0], 3 * wq.shape[1]
        many = wo.shape[1] // cols
        attn = jnp.concatenate([jnp.concatenate([wq, wk, wv], 1)] + [wo[:, i * cols : (i + 1) * cols] for i in range(many)])
        halves = ring_gather(ring_gather(attn[:, : cols // 2], along_y), along_z), ring_gather(ring_gather(attn[:, cols // 2 :], along_z), along_y)
        w_in = whole(beside(w_gate, w_up))
        w_out = whole(w_down)

        tokens = SHARDS * h.shape[0]
        lies_at, holds = orders()
        angle = jnp.arange(tokens, dtype=F32)[:, None] * THETA ** (-jnp.arange(HALF, dtype=F32) / HALF)
        cos, sin = jnp.cos(angle), jnp.sin(angle)

        a_own, norm_a = jax.vjp(normed, h)
        a, d_y, halves = lax.optimization_barrier((gather_tokens(a_own), gather_tokens(dy), halves))
        w_qkv, w_o = attn_shard(halves, tall, low, many)
        qkv = moved(_ordered, lies_at, [matmul(a, w_qkv), cos, sin], [shaped(tokens, cols)])[0]
        out, lse = attend(qkv)
        heads = moved(_copied, holds, [out], [shaped(*out.shape)])[0]
        h = h + scatter_tokens(heads, w_o, 0)
        b_own, norm_b = jax.vjp(normed, h)
        b = gather_tokens(b_own)
        both, hidden = into_hidden(b, w_in)

        d_out_w, w_out = lax.optimization_barrier((row_major(matmul(hidden, d_y, 0, 0)), w_out))
        by_out = summed(d_out_w)
        d_both = hidden_back(d_y, w_out, both)
        d_in_w, d_both = lax.optimization_barrier((row_major(matmul(b, d_both, 0, 0)), d_both))
        by_in = summed(d_in_w)
        d_b, by_out = lax.optimization_barrier((scatter_tokens(d_both, w_in, 1), by_out))
        d_h = dy + norm_b(d_b)[0]
        d_attn = gather_tokens(d_h)
        d_out, delta = moved(_with_delta, lies_at, [matmul(d_attn, w_o, 1, 1), out], [shaped(*out.shape), jax.ShapeDtypeStruct(lse.shape, F32)])
        by_o = row_major(matmul(heads, d_attn, 0, 0))
        d_qkv = moved(_given_back, holds, [*attend_back(qkv, d_out, lse, delta), cos, sin], [shaped(*qkv.shape)])[0]
        first, second = attn_pack(row_major(matmul(a, d_qkv, 0, 0)), by_o)
        first, second, d_qkv = lax.optimization_barrier((first, second, d_qkv))
        first, second, d_a = lax.optimization_barrier((ring_far(first, along_z), ring_far(second, along_y), chip_sum(d_qkv, w_qkv, 1)))
        d_x = d_h + norm_a(place_sum(*d_a))[0]
        first, second = ring_scatter(ring_near(*first, along_z), along_y), ring_scatter(ring_near(*second, along_y), along_z)
        by_attn = jnp.concatenate([first, second], 1).astype(BF16)
        by_o = jnp.concatenate([by_attn[tall + i * low : tall + (i + 1) * low] for i in range(many)], 1)
        return (d_x[None], *jnp.split(by_attn[:tall], 3, 1), by_o, *apart(by_in), by_out)

    states, by_columns, by_rows = P("dp", "tp", None), P("dp", "tp"), P(("tp", "dp"), None)
    weights = (by_columns, by_columns, by_columns, by_rows, by_columns, by_columns, by_rows)
    return jax.shard_map(step, mesh=mesh, in_specs=(states, states, *weights), out_specs=(states, *weights), check_vma=False)
```

```python
import jax
import jax.numpy as jnp
from jax import lax
from jax.experimental import pallas as pl
from jax.experimental.layout import Layout, with_layout_constraint
from jax.experimental.pallas import tpu as pltpu
from jax.sharding import PartitionSpec as P

HEAD = 256
HALF = HEAD // 2
THETA = 10000
LOG2E = 1.4426950408889634
HIDDEN = -2e30
VMEM = 56 * 2**20
STRIP = 256
TILE = 256
SIDE = 4
CORES = 2
SHARDS = SIDE * CORES
PLACES = SIDE * SIDE
BF16, F32 = jnp.bfloat16, jnp.float32


def dot(a, b, ca=1, cb=0):
    return lax.dot_general(a, b, (((ca,), (cb,)), ((), ())), preferred_element_type=F32)


def matmul(a, b, ca=1, cb=0):
    return dot(a, b, ca, cb).astype(BF16)


def row_major(t):
    return with_layout_constraint(t, Layout(major_to_minor=tuple(range(t.ndim))))


def normed(h):
    wide = h.astype(F32)
    scale = lax.rsqrt(jnp.mean(wide**2, -1, keepdims=True) + 1e-6)
    return (wide * scale).astype(BF16)


def shaped(*shape):
    return jax.ShapeDtypeStruct(shape, BF16)


def call(body, grid, ins, outs, tables=(), scratch=(), flops=0):
    moved = sum(t.size * t.dtype.itemsize for t, _, _ in [*ins, *outs])
    return pl.pallas_call(
        body,
        grid_spec=pltpu.PrefetchScalarGridSpec(
            num_scalar_prefetch=len(tables), grid=(grid,), in_specs=[pl.BlockSpec(b, m) for _, b, m in ins],
            out_specs=[pl.BlockSpec(b, m) for _, b, m in outs], scratch_shapes=list(scratch)),
        out_shape=[s for s, _, _ in outs],
        compiler_params=pltpu.CompilerParams(dimension_semantics=("arbitrary",), vmem_limit_bytes=VMEM),
        cost_estimate=pl.CostEstimate(flops=flops or 100 * moved, transcendentals=0, bytes_accessed=moved),
    )(*tables, *[t for t, _, _ in ins])


def all_of(t):
    return t, t.shape, lambda *_: (0,) * len(t.shape)


def _scores(q_ref, k_ref, at):
    seen = at + STRIP
    s = dot(k_ref[:seen, :], q_ref[at:seen, :], 1, 1)
    key, query = (lax.broadcasted_iota(jnp.int32, s.shape, n) for n in range(2))
    return jnp.where(key <= query + at, s, HIDDEN)


def _forward(q_ref, k_ref, v_ref, o_ref, lse_ref):
    scale = HEAD**-0.5
    for at in range(0, q_ref.shape[0], STRIP):
        seen = at + STRIP
        s = _scores(q_ref, k_ref, at)
        top = s.max(axis=0, keepdims=True)
        p = jnp.exp2((s - top) * (scale * LOG2E)).astype(BF16)
        values = jnp.concatenate([v_ref[:seen, :].T, jnp.ones((8, seen), BF16)], axis=0)
        mix = dot(values, p)
        total = mix[HEAD : HEAD + 1, :]
        o_ref[at:seen, :] = (mix[:HEAD, :] * (1 / total)).T.astype(BF16)
        lse_ref[0, :, at:seen] = top * scale + jnp.log(total)


def _backward(q_ref, k_ref, v_ref, do_ref, lse_ref, delta_ref, dq_ref, dk_ref, dv_ref, dk_s, dv_s):
    scale = HEAD**-0.5
    dk_s[...] = jnp.zeros_like(dk_s)
    dv_s[...] = jnp.zeros_like(dv_s)
    for at in range(0, q_ref.shape[0], STRIP):
        seen = at + STRIP
        q, do = q_ref[at:seen, :], do_ref[at:seen, :]
        p = jnp.exp2(_scores(q_ref, k_ref, at) * (scale * LOG2E) - lse_ref[0, :, at:seen] * LOG2E)
        ds = (p * (dot(v_ref[:seen, :], do, 1, 1) - delta_ref[0, :, at:seen])).astype(BF16)
        dv_s[:seen, :] += dot(p.astype(BF16), do)
        dk_s[:seen, :] += dot(ds, q)
        dq_ref[at:seen, :] = (dot(k_ref[:seen, :].T, ds) * scale).T.astype(BF16)
    dk_ref[...] = (dk_s[...] * scale).astype(BF16)
    dv_ref[...] = dv_s[...].astype(BF16)


def attend(qkv):
    s, h = qkv.shape[0], qkv.shape[1] // (3 * HEAD)
    cols = lambda n: (qkv, (s, HEAD), lambda i: (0, n * h + i))
    return call(_forward, h, [cols(0), cols(1), cols(2)],
                [(shaped(s, h * HEAD), (s, HEAD), lambda i: (0, i)), (jax.ShapeDtypeStruct((h, 1, s), F32), (1, 1, s), lambda i: (i, 0, 0))],
                flops=4 * s * s * h * HEAD)


def attend_back(qkv, d_out, lse, delta):
    s, h = qkv.shape[0], qkv.shape[1] // (3 * HEAD)
    cols = lambda n: (qkv, (s, HEAD), lambda i: (0, n * h + i))
    one = lambda t: (t, (s, HEAD), lambda i: (0, i))
    stat = lambda t: (t, (1, 1, s), lambda i: (i, 0, 0))
    return call(_backward, h, [cols(0), cols(1), cols(2), one(d_out), stat(lse), stat(delta)], 3 * [one(shaped(s, h * HEAD))],
                scratch=2 * [pltpu.VMEM((s, HEAD), F32)], flops=10 * s * s * h * HEAD)


def _beside(a_ref, b_ref, out_ref):
    for at in range(0, a_ref.shape[1], TILE):
        out_ref[:, 2 * at : 2 * at + TILE] = a_ref[:, at : at + TILE]
        out_ref[:, 2 * at + TILE : 2 * (at + TILE)] = b_ref[:, at : at + TILE]


def _apart(t_ref, a_ref, b_ref):
    for at in range(0, a_ref.shape[1], TILE):
        a_ref[:, at : at + TILE] = t_ref[:, 2 * at : 2 * at + TILE]
        b_ref[:, at : at + TILE] = t_ref[:, 2 * at + TILE : 2 * (at + TILE)]


def _column(t, wide):
    return t, (t.shape[0], wide), lambda i: (0, i)


def beside(a, b):
    rows, n = a.shape
    return call(_beside, 1, [all_of(a), all_of(b)], [all_of(shaped(rows, 2 * n))])[0]


def apart(t):
    rows, n = t.shape[0], t.shape[1] // 2
    return call(_apart, 1, [all_of(t)], 2 * [all_of(shaped(rows, n))])


def _into(b_ref, w_ref, both_ref, hidden_ref):
    both = dot(b_ref[...], w_ref[...])
    both_ref[...] = both
    hidden_ref[...] = (jax.nn.silu(both[:, :TILE]) * both[:, TILE:]).astype(BF16)


def into_hidden(b, w):
    m, k, n = *b.shape, w.shape[1]
    return call(_into, n // (2 * TILE), [all_of(b), _column(w, 2 * TILE)],
                [_column(jax.ShapeDtypeStruct((m, n), F32), 2 * TILE), _column(shaped(m, n // 2), TILE)], flops=2 * m * k * n)


def _back_into(d_ref, w_ref, both_ref, out_ref):
    d = matmul(d_ref[...], w_ref[...], 1, 1).astype(F32)
    gate, up = both_ref[:, :TILE], both_ref[:, TILE:]
    s = jax.nn.sigmoid(gate)
    out_ref[:, :TILE] = (d * up * (s * (1 + gate * (1 - s)))).astype(BF16)
    out_ref[:, TILE:] = (d * (gate * s)).astype(BF16)


def hidden_back(d, w, both):
    m, k, n = *d.shape, w.shape[0]
    return call(_back_into, n // TILE, [all_of(d), (w, (TILE, k), lambda i: (i, 0)), _column(both, 2 * TILE)],
                [_column(shaped(m, 2 * n), 2 * TILE)], flops=2 * m * k * n)[0]


def along_x(i):
    return "tp", [(t, (t + CORES * i) % SHARDS) for t in range(SHARDS)]


def along_y(i):
    return "dp", [(p, (p + SIDE * i) % PLACES) for p in range(PLACES)]


def along_z(i):
    return "dp", [(p, p // SIDE * SIDE + (p + i) % SIDE) for p in range(PLACES)]


def swap():
    return "tp", [(t, t + 1 - 2 * (t % CORES)) for t in range(SHARDS)]


def send(t, way):
    return lax.ppermute(t, *way)


def gather_tokens(t):
    mine = [t] + [send(t, along_x(-i)) for i in range(1, SIDE)]
    return jnp.concatenate(mine + [send(block, swap()) for block in mine])


def chip_sum(t, w, cw):
    half = t.shape[0] // CORES
    term = matmul(t, w, 1, cw)
    own, *others = jnp.split(term[:half].astype(F32) + send(term[half:], swap()).astype(F32), SIDE)
    return own, [t.astype(BF16) for t in others]


def place_sum(own, others):
    for i, t in enumerate(others):
        own += send(t, along_x(i + 1)).astype(F32)
    return own.astype(BF16)


def scatter_tokens(t, w, cw):
    return place_sum(*chip_sum(t, w, cw))


def orders():
    me = lax.axis_index("tp")
    chip, core = me // CORES, me % CORES
    run = jnp.arange(SHARDS, dtype=jnp.int32)
    lies_at = SIDE * ((run % CORES + core) % CORES) + (run // CORES + SIDE - chip) % SIDE
    holds = CORES * ((run % SIDE + chip) % SIDE) + (run // SIDE + core) % CORES
    return lies_at, holds


def _turn(t, cos, sin):
    done = []
    for at in range(0, t.shape[1], HEAD):
        a, b = t[:, at : at + HALF].astype(F32), t[:, at + HALF : at + HEAD].astype(F32)
        done += [a * cos - b * sin, b * cos + a * sin]
    return jnp.concatenate(done, 1).astype(BF16)


def _runs(at, n):
    return [(pl.ds(pl.multiple_of(at[i] * n, n), n), slice(i * n, (i + 1) * n)) for i in range(SHARDS)]


def _ordered(at, t_ref, cos_ref, sin_ref, out_ref):
    turned = 2 * t_ref.shape[1] // 3
    for there, here in _runs(at, t_ref.shape[0] // SHARDS):
        out_ref[here, :turned] = _turn(t_ref[there, :turned], cos_ref[here, :], sin_ref[here, :])
        out_ref[here, turned:] = t_ref[there, turned:]


def _given_back(at, q_ref, k_ref, v_ref, cos_ref, sin_ref, out_ref):
    n = q_ref.shape[1]
    for there, here in _runs(at, q_ref.shape[0] // SHARDS):
        cos, sin = cos_ref[there, :], -sin_ref[there, :]
        out_ref[here, :n] = _turn(q_ref[there, :], cos, sin)
        out_ref[here, n : 2 * n] = _turn(k_ref[there, :], cos, sin)
        out_ref[here, 2 * n :] = v_ref[there, :]


def _copied(at, t_ref, out_ref):
    for there, here in _runs(at, t_ref.shape[0] // SHARDS):
        out_ref[here, :] = t_ref[there, :]


def _with_delta(at, do_ref, o_ref, out_ref, delta_ref):
    for there, here in _runs(at, do_ref.shape[0] // SHARDS):
        do = do_ref[there, :]
        out_ref[here, :] = do
        both = do.astype(F32) * o_ref[here, :].astype(F32)
        for n in range(delta_ref.shape[0]):
            delta_ref[n, :, here] = both[:, n * HEAD : (n + 1) * HEAD].T.sum(axis=0, keepdims=True)


def moved(body, table, ins, outs):
    return call(body, 1, [all_of(t) for t in ins], [all_of(t) for t in outs], (table,))


def ring_gather(t, way):
    half = t.shape[0] // 2
    before, after = send(t, way(1)), send(t, way(-1))
    return jnp.concatenate([t, after, send(before[:half], way(1)), send(after[half:], way(-1)), before])


def ring_far(t, way):
    half = t.shape[0] // (2 * SIDE)
    far = t[2 * 2 * half : 3 * 2 * half].astype(BF16)
    return t, send(far[:half], way(1)), send(far[half:], way(-1))


def ring_near(t, before, after, way):
    rows = t.shape[0] // SIDE
    half = rows // 2
    own, right, _, left = (t[n * rows : (n + 1) * rows] for n in range(SIDE))
    add = lambda a, b: (a.astype(F32) + b.astype(F32)).astype(BF16)
    right = jnp.concatenate([add(right[:half], before), right[half:].astype(BF16)])
    left = jnp.concatenate([left[:half].astype(BF16), add(left[half:], after)])
    return own.astype(F32) + send(right, way(1)).astype(F32) + send(left, way(-1)).astype(F32)


def ring_sum(t, way):
    rows = t.shape[0] // SIDE
    own = t[:rows].astype(F32)
    for n in range(1, SIDE):
        own += send(t[n * rows : (n + 1) * rows].astype(BF16), way(n)).astype(F32)
    return own


def places():
    me = lax.axis_index("dp")
    y, z = me // SIDE, me % SIDE
    n = jnp.arange(PLACES, dtype=jnp.int32)
    high, low = n // SIDE, n % SIDE
    dy, dz = (high + SIDE - y) % SIDE, (low + SIDE - z) % SIDE
    return (SIDE * dz + dy, SIDE * dy + dz), (SIDE * ((low + y) % SIDE) + (high + z) % SIDE, SIDE * ((high + y) % SIDE) + (low + z) % SIDE)


def _placed(*refs):
    halves, (qkv_ref, o_ref) = refs[2:4], refs[4:]
    tall, low = qkv_ref.shape[0], o_ref.shape[0]
    wide = halves[0].shape[1]
    for n, ref in enumerate(halves):
        qkv_ref[:, n * wide : (n + 1) * wide] = ref[:tall, :]
        for i in range(o_ref.shape[1] // (2 * wide)):
            o_ref[:, (2 * i + n) * wide : (2 * i + n + 1) * wide] = ref[tall + i * low : tall + (i + 1) * low, :]


def attn_shard(halves, tall, low, many):
    cols = 2 * halves[0].shape[1]
    block = (tall + low * many, cols // 2)
    return call(_placed, PLACES, [(halves[0], block, lambda i, a, b: (a[i], 0)), (halves[1], block, lambda i, a, b: (b[i], 0))],
                [(shaped(PLACES * tall, cols), (tall, cols), lambda i, a, b: (i, 0)), (shaped(PLACES * low, cols * many), (low, cols * many), lambda i, a, b: (i, 0))],
                places()[0])


def _packed(first, second, qkv_ref, o_ref, *outs):
    tall, low = qkv_ref.shape[0] // PLACES, o_ref.shape[0] // PLACES
    spots = PLACES // pl.num_programs(0)
    for n, (at, ref) in enumerate(zip((first, second), outs)):
        wide = ref.shape[1]
        for spot in range(PLACES // SIDE):
            place = at[pl.program_id(0) * spots + spot]
            row = spot * (ref.shape[0] // SIDE)
            ref[row : row + tall, :] = qkv_ref[pl.ds(pl.multiple_of(place * tall, tall), tall), n * wide : (n + 1) * wide]
            row += tall
            for i in range(o_ref.shape[1] // (2 * wide)):
                ref[row : row + low, :] = o_ref[pl.ds(pl.multiple_of(place * low, low), low), (2 * i + n) * wide : (2 * i + n + 1) * wide]
                row += low


def attn_pack(by_qkv, by_o):
    wide = by_qkv.shape[1] // 2
    rows = (by_qkv.size + by_o.size) // (2 * wide)
    return call(_packed, SIDE, [all_of(by_qkv), all_of(by_o)], 2 * [(shaped(rows, wide), (rows // SIDE, wide), lambda i, *_: (i, 0))], places()[1])


def solution(mesh):
    def whole(t):
        return lax.all_gather(t, "dp", axis=0, tiled=True)

    def summed(t):
        return lax.psum_scatter(t, "dp", scatter_dimension=0, tiled=True)

    def step(x, dy, wq, wk, wv, wo, w_gate, w_up, w_down):
        h, dy = x[0], dy[0]
        tall, low, cols = wq.shape[0], wo.shape[0], 3 * wq.shape[1]
        many = wo.shape[1] // cols
        attn = jnp.concatenate([jnp.concatenate([wq, wk, wv], 1)] + [wo[:, i * cols : (i + 1) * cols] for i in range(many)])
        halves = ring_gather(ring_gather(attn[:, : cols // 2], along_y), along_z), ring_gather(ring_gather(attn[:, cols // 2 :], along_z), along_y)
        w_in = whole(beside(w_gate, w_up))
        w_out = whole(w_down)

        tokens = SHARDS * h.shape[0]
        lies_at, holds = orders()
        angle = jnp.arange(tokens, dtype=F32)[:, None] * THETA ** (-jnp.arange(HALF, dtype=F32) / HALF)
        cos, sin = jnp.cos(angle), jnp.sin(angle)

        a_own, norm_a = jax.vjp(normed, h)
        a, d_y, halves = lax.optimization_barrier((gather_tokens(a_own), gather_tokens(dy), halves))
        w_qkv, w_o = attn_shard(halves, tall, low, many)
        qkv = moved(_ordered, lies_at, [matmul(a, w_qkv), cos, sin], [shaped(tokens, cols)])[0]
        out, lse = attend(qkv)
        heads = moved(_copied, holds, [out], [shaped(*out.shape)])[0]
        h = h + scatter_tokens(heads, w_o, 0)
        b_own, norm_b = jax.vjp(normed, h)
        b = gather_tokens(b_own)
        both, hidden = into_hidden(b, w_in)

        d_out_w, w_out = lax.optimization_barrier((row_major(matmul(hidden, d_y, 0, 0)), w_out))
        by_out = summed(d_out_w)
        d_both = hidden_back(d_y, w_out, both)
        d_in_w, d_both = lax.optimization_barrier((row_major(matmul(b, d_both, 0, 0)), d_both))
        by_in = summed(d_in_w)
        d_b, by_out = lax.optimization_barrier((scatter_tokens(d_both, w_in, 1), by_out))
        d_h = dy + norm_b(d_b)[0]
        d_attn = gather_tokens(d_h)
        d_out, delta = moved(_with_delta, lies_at, [matmul(d_attn, w_o, 1, 1), out], [shaped(*out.shape), jax.ShapeDtypeStruct(lse.shape, F32)])
        by_o = row_major(matmul(heads, d_attn, 0, 0))
        d_qkv = moved(_given_back, holds, [*attend_back(qkv, d_out, lse, delta), cos, sin], [shaped(*qkv.shape)])[0]
        first, second = attn_pack(row_major(matmul(a, d_qkv, 0, 0)), by_o)
        first, second, d_qkv = lax.optimization_barrier((first, second, d_qkv))
        first, second = ring_far(first, along_z), ring_far(second, along_y)
        d_a = chip_sum(d_qkv, w_qkv, 1)
        first, second, d_a = lax.optimization_barrier((first, second, d_a))
        d_x = d_h + norm_a(place_sum(*d_a))[0]
        first, second = ring_sum(ring_near(*first, along_z), along_y), ring_sum(ring_near(*second, along_y), along_z)
        by_attn = jnp.concatenate([first, second], 1).astype(BF16)
        by_o = jnp.concatenate([by_attn[tall + i * low : tall + (i + 1) * low] for i in range(many)], 1)
        return (d_x[None], *jnp.split(by_attn[:tall], 3, 1), by_o, *apart(by_in), by_out)

    states, by_columns, by_rows = P("dp", "tp", None), P("dp", "tp"), P(("tp", "dp"), None)
    weights = (by_columns, by_columns, by_columns, by_rows, by_columns, by_columns, by_rows)
    step = jax.shard_map(step, mesh=mesh, in_specs=(states, states, *weights), out_specs=(states, *weights), check_vma=False)
    return step
```

```python
import jax
import jax.numpy as jnp
from jax import lax
from jax.experimental import pallas as pl
from jax.experimental.layout import Layout, with_layout_constraint
from jax.experimental.pallas import tpu as pltpu
from jax.sharding import PartitionSpec as P

HEAD = 256
HALF = HEAD // 2
THETA = 10000
LOG2E = 1.4426950408889634
HIDDEN = -2e30
VMEM = 56 * 2**20
STRIP = 256
TILE = 256
SIDE = 4
CORES = 2
SHARDS = SIDE * CORES
PLACES = SIDE * SIDE
BF16, F32 = jnp.bfloat16, jnp.float32


def dot(a, b, ca=1, cb=0):
    return lax.dot_general(a, b, (((ca,), (cb,)), ((), ())), preferred_element_type=F32)


def matmul(a, b, ca=1, cb=0):
    return dot(a, b, ca, cb).astype(BF16)


def row_major(t):
    return with_layout_constraint(t, Layout(major_to_minor=tuple(range(t.ndim))))


def normed(h):
    wide = h.astype(F32)
    scale = lax.rsqrt(jnp.mean(wide**2, -1, keepdims=True) + 1e-6)
    return (wide * scale).astype(BF16)


def shaped(*shape):
    return jax.ShapeDtypeStruct(shape, BF16)


def call(body, grid, ins, outs, tables=(), scratch=(), flops=0):
    moved = sum(t.size * t.dtype.itemsize for t, _, _ in [*ins, *outs])
    return pl.pallas_call(
        body,
        grid_spec=pltpu.PrefetchScalarGridSpec(
            num_scalar_prefetch=len(tables), grid=(grid,), in_specs=[pl.BlockSpec(b, m) for _, b, m in ins],
            out_specs=[pl.BlockSpec(b, m) for _, b, m in outs], scratch_shapes=list(scratch)),
        out_shape=[s for s, _, _ in outs],
        compiler_params=pltpu.CompilerParams(dimension_semantics=("arbitrary",), vmem_limit_bytes=VMEM),
        cost_estimate=pl.CostEstimate(flops=flops or 100 * moved, transcendentals=0, bytes_accessed=moved),
    )(*tables, *[t for t, _, _ in ins])


def all_of(t):
    return t, t.shape, lambda *_: (0,) * len(t.shape)


def _scores(q_ref, k_ref, at):
    seen = at + STRIP
    s = dot(k_ref[:seen, :], q_ref[at:seen, :], 1, 1)
    key, query = (lax.broadcasted_iota(jnp.int32, s.shape, n) for n in range(2))
    return jnp.where(key <= query + at, s, HIDDEN)


def _forward(q_ref, k_ref, v_ref, o_ref, lse_ref):
    scale = HEAD**-0.5
    for at in range(0, q_ref.shape[0], STRIP):
        seen = at + STRIP
        s = _scores(q_ref, k_ref, at)
        top = s.max(axis=0, keepdims=True)
        p = jnp.exp2((s - top) * (scale * LOG2E)).astype(BF16)
        values = jnp.concatenate([v_ref[:seen, :].T, jnp.ones((8, seen), BF16)], axis=0)
        mix = dot(values, p)
        total = mix[HEAD : HEAD + 1, :]
        o_ref[at:seen, :] = (mix[:HEAD, :] * (1 / total)).T.astype(BF16)
        lse_ref[0, :, at:seen] = top * scale + jnp.log(total)


def _backward(q_ref, k_ref, v_ref, do_ref, lse_ref, delta_ref, dq_ref, dk_ref, dv_ref, dk_s, dv_s):
    scale = HEAD**-0.5
    dk_s[...] = jnp.zeros_like(dk_s)
    dv_s[...] = jnp.zeros_like(dv_s)
    for at in range(0, q_ref.shape[0], STRIP):
        seen = at + STRIP
        q, do = q_ref[at:seen, :], do_ref[at:seen, :]
        p = jnp.exp2(_scores(q_ref, k_ref, at) * (scale * LOG2E) - lse_ref[0, :, at:seen] * LOG2E)
        ds = (p * (dot(v_ref[:seen, :], do, 1, 1) - delta_ref[0, :, at:seen])).astype(BF16)
        dv_s[:seen, :] += dot(p.astype(BF16), do)
        dk_s[:seen, :] += dot(ds, q)
        dq_ref[at:seen, :] = (dot(k_ref[:seen, :].T, ds) * scale).T.astype(BF16)
    dk_ref[...] = (dk_s[...] * scale).astype(BF16)
    dv_ref[...] = dv_s[...].astype(BF16)


def attend(qkv):
    s, h = qkv.shape[0], qkv.shape[1] // (3 * HEAD)
    cols = lambda n: (qkv, (s, HEAD), lambda i: (0, n * h + i))
    return call(_forward, h, [cols(0), cols(1), cols(2)],
                [(shaped(s, h * HEAD), (s, HEAD), lambda i: (0, i)), (jax.ShapeDtypeStruct((h, 1, s), F32), (1, 1, s), lambda i: (i, 0, 0))],
                flops=4 * s * s * h * HEAD)


def attend_back(qkv, d_out, lse, delta):
    s, h = qkv.shape[0], qkv.shape[1] // (3 * HEAD)
    cols = lambda n: (qkv, (s, HEAD), lambda i: (0, n * h + i))
    one = lambda t: (t, (s, HEAD), lambda i: (0, i))
    stat = lambda t: (t, (1, 1, s), lambda i: (i, 0, 0))
    return call(_backward, h, [cols(0), cols(1), cols(2), one(d_out), stat(lse), stat(delta)], 3 * [one(shaped(s, h * HEAD))],
                scratch=2 * [pltpu.VMEM((s, HEAD), F32)], flops=10 * s * s * h * HEAD)


def _beside(a_ref, b_ref, out_ref):
    for at in range(0, a_ref.shape[1], TILE):
        out_ref[:, 2 * at : 2 * at + TILE] = a_ref[:, at : at + TILE]
        out_ref[:, 2 * at + TILE : 2 * (at + TILE)] = b_ref[:, at : at + TILE]


def _apart(t_ref, a_ref, b_ref):
    for at in range(0, a_ref.shape[1], TILE):
        a_ref[:, at : at + TILE] = t_ref[:, 2 * at : 2 * at + TILE]
        b_ref[:, at : at + TILE] = t_ref[:, 2 * at + TILE : 2 * (at + TILE)]


def _column(t, wide):
    return t, (t.shape[0], wide), lambda i: (0, i)


def beside(a, b):
    rows, n = a.shape
    return call(_beside, 1, [all_of(a), all_of(b)], [all_of(shaped(rows, 2 * n))])[0]


def apart(t):
    rows, n = t.shape[0], t.shape[1] // 2
    return call(_apart, 1, [all_of(t)], 2 * [all_of(shaped(rows, n))])


def _into(b_ref, w_ref, both_ref, hidden_ref):
    both = dot(b_ref[...], w_ref[...])
    both_ref[...] = both
    hidden_ref[...] = (jax.nn.silu(both[:, :TILE]) * both[:, TILE:]).astype(BF16)


def into_hidden(b, w):
    m, k, n = *b.shape, w.shape[1]
    return call(_into, n // (2 * TILE), [all_of(b), _column(w, 2 * TILE)],
                [_column(jax.ShapeDtypeStruct((m, n), F32), 2 * TILE), _column(shaped(m, n // 2), TILE)], flops=2 * m * k * n)


def _back_into(d_ref, w_ref, both_ref, out_ref):
    d = matmul(d_ref[...], w_ref[...], 1, 1).astype(F32)
    gate, up = both_ref[:, :TILE], both_ref[:, TILE:]
    s = jax.nn.sigmoid(gate)
    out_ref[:, :TILE] = (d * up * (s * (1 + gate * (1 - s)))).astype(BF16)
    out_ref[:, TILE:] = (d * (gate * s)).astype(BF16)


def hidden_back(d, w, both):
    m, k, n = *d.shape, w.shape[0]
    return call(_back_into, n // TILE, [all_of(d), (w, (TILE, k), lambda i: (i, 0)), _column(both, 2 * TILE)],
                [_column(shaped(m, 2 * n), 2 * TILE)], flops=2 * m * k * n)[0]


def along_x(i):
    return "tp", [(t, (t + CORES * i) % SHARDS) for t in range(SHARDS)]


def along_y(i):
    return "dp", [(p, (p + SIDE * i) % PLACES) for p in range(PLACES)]


def along_z(i):
    return "dp", [(p, p // SIDE * SIDE + (p + i) % SIDE) for p in range(PLACES)]


def swap():
    return "tp", [(t, t + 1 - 2 * (t % CORES)) for t in range(SHARDS)]


def send(t, way):
    return lax.ppermute(t, *way)


def gather_tokens(t):
    mine = [t] + [send(t, along_x(-i)) for i in range(1, SIDE)]
    return jnp.concatenate(mine + [send(block, swap()) for block in mine])


def chip_sum(t, w, cw):
    half = t.shape[0] // CORES
    term = matmul(t, w, 1, cw)
    own, *others = jnp.split(term[:half].astype(F32) + send(term[half:], swap()).astype(F32), SIDE)
    return own, [t.astype(BF16) for t in others]


def place_sum(own, others):
    for i, t in enumerate(others):
        own += send(t, along_x(i + 1)).astype(F32)
    return own.astype(BF16)


def scatter_tokens(t, w, cw):
    return place_sum(*chip_sum(t, w, cw))


def orders():
    me = lax.axis_index("tp")
    chip, core = me // CORES, me % CORES
    run = jnp.arange(SHARDS, dtype=jnp.int32)
    lies_at = SIDE * ((run % CORES + core) % CORES) + (run // CORES + SIDE - chip) % SIDE
    holds = CORES * ((run % SIDE + chip) % SIDE) + (run // SIDE + core) % CORES
    return lies_at, holds


def _turn(t, cos, sin):
    done = []
    for at in range(0, t.shape[1], HEAD):
        a, b = t[:, at : at + HALF].astype(F32), t[:, at + HALF : at + HEAD].astype(F32)
        done += [a * cos - b * sin, b * cos + a * sin]
    return jnp.concatenate(done, 1).astype(BF16)


def _runs(at, n):
    return [(pl.ds(pl.multiple_of(at[i] * n, n), n), slice(i * n, (i + 1) * n)) for i in range(SHARDS)]


def _ordered(at, t_ref, cos_ref, sin_ref, out_ref):
    turned = 2 * t_ref.shape[1] // 3
    for there, here in _runs(at, t_ref.shape[0] // SHARDS):
        out_ref[here, :turned] = _turn(t_ref[there, :turned], cos_ref[here, :], sin_ref[here, :])
        out_ref[here, turned:] = t_ref[there, turned:]


def _given_back(at, q_ref, k_ref, v_ref, cos_ref, sin_ref, out_ref):
    n = q_ref.shape[1]
    for there, here in _runs(at, q_ref.shape[0] // SHARDS):
        cos, sin = cos_ref[there, :], -sin_ref[there, :]
        out_ref[here, :n] = _turn(q_ref[there, :], cos, sin)
        out_ref[here, n : 2 * n] = _turn(k_ref[there, :], cos, sin)
        out_ref[here, 2 * n :] = v_ref[there, :]


def _copied(at, t_ref, out_ref):
    for there, here in _runs(at, t_ref.shape[0] // SHARDS):
        out_ref[here, :] = t_ref[there, :]


def _with_delta(at, do_ref, o_ref, out_ref, delta_ref):
    for there, here in _runs(at, do_ref.shape[0] // SHARDS):
        do = do_ref[there, :]
        out_ref[here, :] = do
        both = do.astype(F32) * o_ref[here, :].astype(F32)
        for n in range(delta_ref.shape[0]):
            delta_ref[n, :, here] = both[:, n * HEAD : (n + 1) * HEAD].T.sum(axis=0, keepdims=True)


def moved(body, table, ins, outs):
    return call(body, 1, [all_of(t) for t in ins], [all_of(t) for t in outs], (table,))


def ring_gather(t, way):
    half = t.shape[0] // 2
    before, after = send(t, way(1)), send(t, way(-1))
    return jnp.concatenate([t, after, send(before[:half], way(1)), send(after[half:], way(-1)), before])


def ring_far(t, way):
    half = t.shape[0] // (2 * SIDE)
    far = t[2 * 2 * half : 3 * 2 * half].astype(BF16)
    return t, send(far[:half], way(1)), send(far[half:], way(-1))


def ring_near(t, before, after, way):
    rows = t.shape[0] // SIDE
    half = rows // 2
    own, right, _, left = (t[n * rows : (n + 1) * rows] for n in range(SIDE))
    add = lambda a, b: (a.astype(F32) + b.astype(F32)).astype(BF16)
    right = jnp.concatenate([add(right[:half], before), right[half:].astype(BF16)])
    left = jnp.concatenate([left[:half].astype(BF16), add(left[half:], after)])
    return own.astype(F32) + send(right, way(1)).astype(F32) + send(left, way(-1)).astype(F32)


def ring_sum(t, way):
    rows = t.shape[0] // SIDE
    own = t[:rows].astype(F32)
    for n in range(1, SIDE):
        own += send(t[n * rows : (n + 1) * rows].astype(BF16), way(n)).astype(F32)
    return own


def places():
    me = lax.axis_index("dp")
    y, z = me // SIDE, me % SIDE
    n = jnp.arange(PLACES, dtype=jnp.int32)
    high, low = n // SIDE, n % SIDE
    dy, dz = (high + SIDE - y) % SIDE, (low + SIDE - z) % SIDE
    return (SIDE * dz + dy, SIDE * dy + dz), (SIDE * ((low + y) % SIDE) + (high + z) % SIDE, SIDE * ((high + y) % SIDE) + (low + z) % SIDE)


def _placed(*refs):
    halves, (qkv_ref, o_ref) = refs[2:4], refs[4:]
    tall, low = qkv_ref.shape[0], o_ref.shape[0]
    wide = halves[0].shape[1]
    for n, ref in enumerate(halves):
        qkv_ref[:, n * wide : (n + 1) * wide] = ref[:tall, :]
        for i in range(o_ref.shape[1] // (2 * wide)):
            o_ref[:, (2 * i + n) * wide : (2 * i + n + 1) * wide] = ref[tall + i * low : tall + (i + 1) * low, :]


def attn_shard(halves, tall, low, many):
    cols = 2 * halves[0].shape[1]
    block = (tall + low * many, cols // 2)
    return call(_placed, PLACES, [(halves[0], block, lambda i, a, b: (a[i], 0)), (halves[1], block, lambda i, a, b: (b[i], 0))],
                [(shaped(PLACES * tall, cols), (tall, cols), lambda i, a, b: (i, 0)), (shaped(PLACES * low, cols * many), (low, cols * many), lambda i, a, b: (i, 0))],
                places()[0])


def _packed(first, second, qkv_ref, o_ref, *outs):
    tall, low = qkv_ref.shape[0] // PLACES, o_ref.shape[0] // PLACES
    spots = PLACES // pl.num_programs(0)
    for n, (at, ref) in enumerate(zip((first, second), outs)):
        wide = ref.shape[1]
        for spot in range(PLACES // SIDE):
            place = at[pl.program_id(0) * spots + spot]
            row = spot * (ref.shape[0] // SIDE)
            ref[row : row + tall, :] = qkv_ref[pl.ds(pl.multiple_of(place * tall, tall), tall), n * wide : (n + 1) * wide]
            row += tall
            for i in range(o_ref.shape[1] // (2 * wide)):
                ref[row : row + low, :] = o_ref[pl.ds(pl.multiple_of(place * low, low), low), (2 * i + n) * wide : (2 * i + n + 1) * wide]
                row += low


def attn_pack(by_qkv, by_o):
    wide = by_qkv.shape[1] // 2
    rows = (by_qkv.size + by_o.size) // (2 * wide)
    return call(_packed, SIDE, [all_of(by_qkv), all_of(by_o)], 2 * [(shaped(rows, wide), (rows // SIDE, wide), lambda i, *_: (i, 0))], places()[1])


def _part_packed(first, second, t_ref, *outs):
    tall = t_ref.shape[0] // PLACES
    for n, (at, ref) in enumerate(zip((first, second), outs)):
        wide = ref.shape[1]
        for spot in range(PLACES // SIDE):
            place = at[pl.program_id(0) * SIDE + spot]
            ref[spot * tall : (spot + 1) * tall, :] = t_ref[pl.ds(pl.multiple_of(place * tall, tall), tall), n * wide : (n + 1) * wide]


def part_pack(t):
    rows, wide = t.shape[0], t.shape[1] // 2
    return call(_part_packed, SIDE, [all_of(t)], 2 * [(shaped(rows, wide), (rows // SIDE, wide), lambda i, *_: (i, 0))], places()[1])


def solution(mesh):
    def whole(t):
        return lax.all_gather(t, "dp", axis=0, tiled=True)

    def summed(t):
        return lax.psum_scatter(t, "dp", scatter_dimension=0, tiled=True)

    def step(x, dy, wq, wk, wv, wo, w_gate, w_up, w_down):
        h, dy = x[0], dy[0]
        tall, low, cols = wq.shape[0], wo.shape[0], 3 * wq.shape[1]
        many = wo.shape[1] // cols
        attn = jnp.concatenate([jnp.concatenate([wq, wk, wv], 1)] + [wo[:, i * cols : (i + 1) * cols] for i in range(many)])
        halves = ring_gather(ring_gather(attn[:, : cols // 2], along_y), along_z), ring_gather(ring_gather(attn[:, cols // 2 :], along_z), along_y)
        w_in = whole(beside(w_gate, w_up))
        w_out = whole(w_down)

        tokens = SHARDS * h.shape[0]
        lies_at, holds = orders()
        angle = jnp.arange(tokens, dtype=F32)[:, None] * THETA ** (-jnp.arange(HALF, dtype=F32) / HALF)
        cos, sin = jnp.cos(angle), jnp.sin(angle)

        a_own, norm_a = jax.vjp(normed, h)
        a, d_y, halves = lax.optimization_barrier((gather_tokens(a_own), gather_tokens(dy), halves))
        w_qkv, w_o = attn_shard(halves, tall, low, many)
        qkv = moved(_ordered, lies_at, [matmul(a, w_qkv), cos, sin], [shaped(tokens, cols)])[0]
        out, lse = attend(qkv)
        heads = moved(_copied, holds, [out], [shaped(*out.shape)])[0]
        h = h + scatter_tokens(heads, w_o, 0)
        b_own, norm_b = jax.vjp(normed, h)
        b = gather_tokens(b_own)
        both, hidden = into_hidden(b, w_in)

        most = d_y.shape[1] - d_y.shape[1] // 3
        one, two = part_pack(row_major(matmul(hidden, d_y[:, most:], 0, 0)))
        d_out_w, one, two = lax.optimization_barrier((row_major(matmul(hidden, d_y[:, :most], 0, 0)), one, two))
        by_out = summed(d_out_w)
        one, two, w_out = lax.optimization_barrier((ring_far(one, along_z), ring_far(two, along_y), w_out))
        d_both = hidden_back(d_y, w_out, both)
        one, two, d_both = lax.optimization_barrier((ring_near(*one, along_z), ring_near(*two, along_y), d_both))
        d_in_w, d_both, one, two = lax.optimization_barrier((row_major(matmul(b, d_both, 0, 0)), d_both, ring_sum(one, along_y), ring_sum(two, along_z)))
        by_part = jnp.concatenate([one, two], 1).astype(BF16)
        by_in = summed(d_in_w)
        d_b, by_out = lax.optimization_barrier((scatter_tokens(d_both, w_in, 1), by_out))
        d_h = dy + norm_b(d_b)[0]
        d_attn = gather_tokens(d_h)
        d_out, delta = moved(_with_delta, lies_at, [matmul(d_attn, w_o, 1, 1), out], [shaped(*out.shape), jax.ShapeDtypeStruct(lse.shape, F32)])
        by_o = row_major(matmul(heads, d_attn, 0, 0))
        d_qkv = moved(_given_back, holds, [*attend_back(qkv, d_out, lse, delta), cos, sin], [shaped(*qkv.shape)])[0]
        first, second = attn_pack(row_major(matmul(a, d_qkv, 0, 0)), by_o)
        first, second, d_qkv = lax.optimization_barrier((first, second, d_qkv))
        first, second = ring_far(first, along_z), ring_far(second, along_y)
        d_a = chip_sum(d_qkv, w_qkv, 1)
        first, second, d_a = lax.optimization_barrier((first, second, d_a))
        d_x = d_h + norm_a(place_sum(*d_a))[0]
        first, second = ring_sum(ring_near(*first, along_z), along_y), ring_sum(ring_near(*second, along_y), along_z)
        by_attn = jnp.concatenate([first, second], 1).astype(BF16)
        by_o = jnp.concatenate([by_attn[tall + i * low : tall + (i + 1) * low] for i in range(many)], 1)
        return (d_x[None], *jnp.split(by_attn[:tall], 3, 1), by_o, *apart(by_in), jnp.concatenate([by_out, by_part], 1))

    states, by_columns, by_rows = P("dp", "tp", None), P("dp", "tp"), P(("tp", "dp"), None)
    weights = (by_columns, by_columns, by_columns, by_rows, by_columns, by_columns, by_rows)
    step = jax.shard_map(step, mesh=mesh, in_specs=(states, states, *weights), out_specs=(states, *weights), check_vma=False)
    return step
```
